32 devices in a mesh: seq: 8 (over z, y), head: 4 (over x, core).
Axes of the slice: x: 2, y: 2, z: 4, core: 2. Of those that a mesh axis runs over, the one named last changes fastest.
Arguments:
- queries: bfloat16 [4096, 12288], P(('seq', 'head')), may hold values from -8 to 8
- latent: bfloat16 [4096, 512], P(('seq', 'head')), may hold values from -6 to 6
- rope_keys: bfloat16 [4096, 64], P(('seq', 'head')), may hold values from -8 to 8
- key_weight: bfloat16 [512, 8192], P('seq', 'head'), may hold values from -0.25 to 0.25
- value_weight: bfloat16 [512, 8192], P('seq', 'head'), may hold values from -0.25 to 0.25
- doc_lengths: int32 [32], replicated, may hold values from 1 to 254, as said below
Outputs:
- attended: bfloat16 [4096, 8192], P(('seq', 'head'))
The draws below stay inside these ranges and needn't reach their ends.
Inputs may be any that keep to these rules, and one draw needn't show every extreme that they name: `doc_lengths`: the documents lie in order in the pack and their lengths sum to 4096; document 0 starts at position 0 and every other document d starts strictly inside positions d * 128 to (d + 1) * 128 - 1, excluding the first of these; one length is exactly 254.
All inputs are finite; a program needn't handle non-finite values.
Results may differ from the reference program's by a relative error of at most 0.0062.
Values may be sent and summed in bfloat16 or wider, within the bound.
A program may use at most 128 MiB of HBM per device.

```python
import math
import jax
import jax.numpy as jnp
from jax import lax

KV_RANK = 512
NOPE = 128
ROPE = 64
VDIM = 128
HEADS = 64
TOK_DEV = 128
TOKENS = 4096
DOCS = 32
N_HEAD = 4


def draw_queries(key, part):
    shape = (TOKENS, HEADS, NOPE + ROPE)
    own_key = jax.random.fold_in(key, 11)
    drawn = jnp.clip(2.0 * jax.random.normal(own_key, shape, jnp.float32), -8.0, 8.0)
    return drawn.reshape(TOKENS, HEADS * (NOPE + ROPE)).astype(jnp.bfloat16)


def draw_rope_keys(key, part):
    shape = (TOKENS, ROPE)
    own_key = jax.random.fold_in(key, 12)
    drawn = jnp.clip(jax.random.normal(own_key, shape, jnp.float32), -8.0, 8.0)
    return drawn.astype(jnp.bfloat16)


def draw_doc_lengths(key, part):
    slot_rows = TOKENS // DOCS
    jitter = jax.random.randint(jax.random.fold_in(key, 21), (DOCS,), 1, slot_rows)
    chosen = jax.random.randint(jax.random.fold_in(key, 22), (), 1, DOCS - 1)
    index = jnp.arange(DOCS, dtype=jnp.int32)
    jitter = jnp.where(index == 1, jnp.minimum(jitter, slot_rows - 2), jitter)
    jitter = jnp.where(index == chosen, 1, jitter)
    jitter = jnp.where(index == chosen + 1, slot_rows - 1, jitter)
    jitter = jnp.where(index == 0, 0, jitter)
    starts = index * slot_rows + jitter
    ends = jnp.concatenate([starts[1:], jnp.full((1,), TOKENS, jnp.int32)])
    return (ends - starts).astype(jnp.int32)


def steps_of(key, dims, cuts, low, high):
    factor_of, own = 1.0, jax.random.fold_in(key, 6)
    for position, shards_of in cuts:
        heights = jnp.exp(jax.random.uniform(jax.random.fold_in(own, position), (shards_of,), jnp.float32, low / len(cuts), high / len(cuts)))
        factor_of = factor_of * jnp.repeat(heights, dims[position] // shards_of).reshape([-1 if axis == position else 1 for axis in range(len(dims))])
    return factor_of


def scatter_about(stream_key, extent, spread, bound, pieces=(), held_as=jnp.bfloat16):
    array = spread * jax.random.normal(stream_key, extent, jnp.float32)
    if pieces:
        array = array * steps_of(stream_key, extent, pieces, -0.22, 0.18)
    return jnp.clip(array, -bound, bound).astype(held_as)


def setup_inputs(seed: int = 0) -> dict:
    key_of = jax.random.split(jax.random.key(seed), 7)
    queries = draw_queries(jax.random.fold_in(key_of[6], 71), 0)
    latent = scatter_about(key_of[1], (TOKENS, KV_RANK), 1.0, 6.0, ((0, 32),))
    rope_keys = draw_rope_keys(jax.random.fold_in(key_of[6], 71), 0)
    key_weight = scatter_about(key_of[3], (KV_RANK, HEADS * NOPE), KV_RANK ** -0.5, 0.25, ((0, 8), (1, 4)))
    value_weight = scatter_about(key_of[4], (KV_RANK, HEADS * VDIM), KV_RANK ** -0.5, 0.25, ((0, 8), (1, 4)))
    doc_lengths = draw_doc_lengths(jax.random.fold_in(key_of[6], 71), 0)
    return dict(queries=queries, latent=latent, rope_keys=rope_keys, key_weight=key_weight, value_weight=value_weight, doc_lengths=doc_lengths)


def reference(queries, latent, rope_keys, key_weight, value_weight, doc_lengths):
    total_rows = queries.shape[0]
    group_rows = TOK_DEV * N_HEAD
    block_rows = min(512, group_rows)
    qk_width = NOPE + ROPE
    key_span = group_rows + block_rows
    score_scale = 1.0 / math.sqrt(qk_width)
    starts = (jnp.cumsum(doc_lengths) - doc_lengths).astype(jnp.int32)
    places = jnp.arange(total_rows, dtype=jnp.int32)
    started = (starts[None, :] <= places[:, None]).astype(jnp.int32)
    doc_of = (lax.optimization_barrier(jnp.sum(started, axis=1)) - 1).astype(jnp.int32)
    keys = jnp.dot(latent, key_weight, preferred_element_type=jnp.float32).astype(jnp.bfloat16)
    values = jnp.dot(latent, value_weight, preferred_element_type=jnp.float32).astype(jnp.bfloat16)
    keys_front = jnp.concatenate([jnp.zeros((group_rows, keys.shape[1]), jnp.bfloat16), keys], axis=0)
    values_front = jnp.concatenate([jnp.zeros((group_rows, values.shape[1]), jnp.bfloat16), values], axis=0)
    rope_front = jnp.concatenate([jnp.zeros((group_rows, ROPE), jnp.bfloat16), rope_keys], axis=0)
    docs_front = jnp.concatenate([-jnp.ones((group_rows,), jnp.int32), doc_of], axis=0)

    def one_block(q_index):
        q_start = (q_index * block_rows).astype(jnp.int32)
        q_block = lax.dynamic_slice_in_dim(queries, q_start, block_rows, 0).astype(jnp.float32)
        q_block = q_block.reshape(block_rows, HEADS, qk_width)
        k_nope = lax.dynamic_slice_in_dim(keys_front, q_start, key_span, 0).astype(jnp.float32)
        k_nope = k_nope.reshape(key_span, HEADS, NOPE)
        k_rope = lax.dynamic_slice_in_dim(rope_front, q_start, key_span, 0).astype(jnp.float32)
        k_values = lax.dynamic_slice_in_dim(values_front, q_start, key_span, 0).astype(jnp.float32)
        k_values = k_values.reshape(key_span, HEADS, VDIM)
        q_docs = lax.dynamic_slice_in_dim(doc_of, q_start, block_rows, 0)
        k_docs = lax.dynamic_slice_in_dim(docs_front, q_start, key_span, 0)
        q_places = q_start + jnp.arange(block_rows, dtype=jnp.int32)
        k_places = q_start - group_rows + jnp.arange(key_span, dtype=jnp.int32)
        scores = jnp.einsum('ihd,jhd->hij', q_block[:, :, :NOPE], k_nope)
        scores = (scores + jnp.einsum('ihd,jd->hij', q_block[:, :, NOPE:], k_rope)) * score_scale
        allowed = (q_docs[:, None] == k_docs[None, :]) & (k_places[None, :] <= q_places[:, None])
        scores = jnp.where(allowed[None, :, :], scores, -jnp.inf)
        row_peak = lax.optimization_barrier(jnp.max(scores, axis=2, keepdims=True))
        expo = jnp.exp(scores - row_peak)
        row_sum = lax.optimization_barrier(jnp.sum(expo, axis=2))
        rounded = lax.optimization_barrier(expo.astype(jnp.bfloat16)).astype(jnp.float32)
        mixed = jnp.einsum('hij,jhd->ihd', rounded, k_values) / jnp.transpose(row_sum)[:, :, None]
        return mixed.reshape(block_rows, HEADS * VDIM).astype(jnp.bfloat16)
    attended = lax.map(one_block, jnp.arange(total_rows // block_rows, dtype=jnp.int32))
    return attended.reshape(total_rows, HEADS * VDIM)
```

```python
import functools
import math

import jax
import jax.numpy as jnp
from jax import lax
from jax.experimental import pallas as pl
from jax.experimental.pallas import tpu as pltpu
from jax.sharding import PartitionSpec as P

NOPE = 128
ROPE = 64
VDIM = 128
QK = NOPE + ROPE
LOG2E = 1.4426950408889634

MESH = pl.DeviceIdType.MESH


def kernel(
    sizes, queries, latrope, key_weight, value_weight, lengths, out,
    lat_all, wk, wv, qbuf, kaug, vbuf, bias, obuf,
    lat_sem, lat_send, mate_send, q_sem, q_send, w_own, w_recv, w_send, o_sem, o_send,
):
    n_seq, n_head, look, chunks, chunk_heads = sizes
    tok, rank = latrope.shape[0], latrope.shape[1] - 2 * ROPE
    rows = key_weight.shape[0]
    half = n_seq // 2
    xs = n_head // 2
    slots = look + n_head
    span = (look + 1) * tok
    cw = chunk_heads * NOPE
    qw = chunk_heads * QK
    seq, head = lax.axis_index("seq"), lax.axis_index("head")
    core, x = head % 2, head // 2
    mate = head + 1 - 2 * core

    odd = seq % 2
    place = (seq // 2) * (1 - odd) + (n_seq - 1 - seq // 2) * odd

    def at_place(where):
        where = (where + n_seq) % n_seq
        fold = where // half
        return 2 * where * (1 - fold) + (2 * (n_seq - 1 - where) + 1) * fold

    after, before = at_place(place + 1), at_place(place - 1)
    next_seq, last_seq = (seq + 1) % n_seq, (seq + n_seq - 1) % n_seq

    barrier = pltpu.get_barrier_semaphore()

    def greet(to_seq, to_head):
        pl.semaphore_signal(barrier, inc=1, device_id=(to_seq, to_head), device_id_type=MESH)

    for k in range(1, n_head):
        greet(seq, (head + k) % n_head)
    greet(after, head)
    greet(before, head)
    for k in range(xs):
        greet(next_seq, ((x + k) % xs) * 2 + core)
        greet(last_seq, ((x + k) % xs) * 2 + core)

    def own_copies():
        pltpu.make_async_copy(latrope, lat_all.at[look + head], lat_sem.at[look + head]).start()
        for c in range(chunks):
            pltpu.make_async_copy(
                queries.at[:, pl.ds(pl.multiple_of(head * chunks * qw + c * qw, 128), qw)],
                qbuf.at[c, head], q_sem.at[c, head],
            ).start()
            for kv, (source, held) in enumerate(((key_weight, wk), (value_weight, wv))):
                pltpu.make_async_copy(
                    source.at[:, pl.ds(c * cw, cw)], held.at[c, seq], w_own.at[c, kv]
                ).start()

    own_copies()
    pl.semaphore_wait(barrier, n_head - 1 + 2 + 2 * xs)

    def lat_copy(k, to_seq, slot):
        return pltpu.make_async_remote_copy(
            src_ref=latrope, dst_ref=lat_all.at[slot],
            send_sem=lat_send.at[k], recv_sem=lat_sem.at[slot],
            device_id=(to_seq, ((x + k % xs) % xs) * 2 + core), device_id_type=MESH,
        )

    def ring_parts(t):
        both = [(0, 0), (0, 1), (1, 0), (1, 1)]
        return both if t < half else [(0, 0), (1, 1)]

    def ring_copy(c, t, way, kv):
        origin = at_place(place - (t - 1)) if way == 0 else at_place(place + (t - 1))
        source, held = ((key_weight, wk), (value_weight, wv))[kv]
        src = source.at[:, pl.ds(c * cw, cw)] if t == 1 else held.at[c, origin]
        index = t - 1
        return pltpu.make_async_remote_copy(
            src_ref=src, dst_ref=held.at[c, origin],
            send_sem=w_send.at[c, index, way, kv], recv_sem=w_recv.at[c, index, way, kv],
            device_id=(after if way == 0 else before, head), device_id_type=MESH,
        )

    def ring_start(c, t):
        for way, kv in ring_parts(t):
            ring_copy(c, t, way, kv).start()

    def ring_take(c, t):
        for way, kv in ring_parts(t):
            origin = at_place(place - t) if way == 0 else at_place(place + t)
            landed = (wk, wv)[kv].at[c, origin]
            pltpu.make_async_copy(landed, landed, w_recv.at[c, t - 1, way, kv]).wait()
            if t + 1 <= half and (way, kv) in ring_parts(t + 1):
                ring_copy(c, t + 1, way, kv).start()

    def q_copy(c, k):
        peer = (head + k) % n_head
        return pltpu.make_async_remote_copy(
            src_ref=queries.at[:, pl.ds(pl.multiple_of(peer * chunks * qw + c * qw, 128), qw)],
            dst_ref=qbuf.at[c, head],
            send_sem=q_send.at[c, k - 1], recv_sem=q_sem.at[c, head],
            device_id=(seq, peer), device_id_type=MESH,
        )

    def o_copy(c, k):
        peer = (head + k) % n_head
        return pltpu.make_async_remote_copy(
            src_ref=obuf.at[c, peer],
            dst_ref=out.at[:, pl.ds(pl.multiple_of(head * chunks * cw + c * cw, 128), cw)],
            send_sem=o_send.at[c, k - 1], recv_sem=o_sem.at[c, head],
            device_id=(seq, peer), device_id_type=MESH,
        )

    def o_own(c):
        return pltpu.make_async_copy(
            obuf.at[c, head],
            out.at[:, pl.ds(pl.multiple_of(head * chunks * cw + c * cw, 128), cw)],
            o_sem.at[c, head],
        )

    for k in range(1, xs):
        lat_copy(k, seq, look + head).start()

    @pl.when(head >= n_head - look)
    def _():
        for k in range(xs):
            lat_copy(xs + k, next_seq, head - (n_head - look)).start()

    for c in range(min(2, chunks)):
        ring_start(c, 1)
    for c in range(chunks):
        for k in range(1, n_head):
            q_copy(c, k).start()

    docs = lengths.shape[0]
    later = lax.broadcasted_iota(jnp.int32, (docs, docs), 1)
    earlier = lax.broadcasted_iota(jnp.int32, (docs, docs), 0)
    starts = jnp.sum(jnp.where(earlier < later, lengths[...], 0), axis=0, keepdims=True)
    first = seq * n_head * tok

    def mask_tile(j, carry):
        q_place = first + j * tok + lax.broadcasted_iota(jnp.int32, (tok, 1), 0)
        begun = jnp.max(jnp.where(starts <= q_place, starts, 0), axis=1, keepdims=True)
        k_place = first + (j - look) * tok + lax.broadcasted_iota(jnp.int32, (tok, span), 1)
        seen = (k_place >= begun) & (k_place <= q_place)
        bias[j] = jnp.where(seen, 0.0, -jnp.inf)
        return carry

    lax.fori_loop(0, n_head, mask_tile, 0)

    def lat_wait(slot):
        pltpu.make_async_copy(lat_all.at[slot], lat_all.at[slot], lat_sem.at[slot]).wait()

    def mate_copy(i):
        slot = 2 * i + core
        return pltpu.make_async_remote_copy(
            src_ref=lat_all.at[slot], dst_ref=lat_all.at[slot],
            send_sem=mate_send.at[i], recv_sem=lat_sem.at[slot],
            device_id=(seq, mate), device_id_type=MESH,
        )

    def lat_all_in():
        for i in list(range(look // 2, slots // 2)) + list(range(look // 2)):
            lat_wait(2 * i + core)
            mate_copy(i).start()
        for i in range(slots // 2):
            lat_wait(2 * i + 1 - core)

    def rope_in():
        lane = lax.broadcasted_iota(jnp.int32, (tok, 2 * ROPE), 1)
        del lane

        def fill(slot, carry):
            tail = lat_all[slot, :, rank:]
            rolled = pltpu.roll(tail.astype(jnp.float32), ROPE, axis=1).astype(jnp.bfloat16)
            at = pl.ds(pl.multiple_of(slot * tok, tok), tok)
            for h in range(chunk_heads):
                kaug[h, at, NOPE:] = tail if h % 2 == 0 else rolled
            return carry

        lax.fori_loop(0, slots, fill, 0)

    block = slots * tok // 2

    def project(c):
        for kv in range(2):
            mine = (wk, wv)[kv].at[c, seq]
            pltpu.make_async_copy(mine, mine, w_own.at[c, kv]).wait()

        def rows_of(i, carry):
            at = pl.ds(pl.multiple_of(i * block, block), block)
            lat = lat_all[pl.ds(i * (slots // 2), slots // 2), :, :rank].reshape(block, rank)
            low = lax.broadcasted_iota(jnp.int32, (block, NOPE), 1) < ROPE
            for pair in range(chunk_heads // 2):
                cols = slice(pair * 2 * NOPE, (pair + 1) * 2 * NOPE)
                w = wk[c, :, :, cols].reshape(rank, 2 * NOPE)
                k = jnp.dot(lat, w, preferred_element_type=jnp.float32)
                kaug[2 * pair, at, :NOPE] = k[:, :NOPE].astype(jnp.bfloat16)
                turned = pltpu.roll(k[:, NOPE:], ROPE, axis=1)
                zeros_first = jnp.where(low, 0.0, turned).astype(jnp.bfloat16)
                kaug[2 * pair + 1, at, :NOPE] = zeros_first
                rope_last = kaug[2 * pair + 1, at, NOPE:].astype(jnp.float32)
                kaug[2 * pair + 1, at, NOPE:] = jnp.where(low, turned, rope_last).astype(
                    jnp.bfloat16
                )
                w = wv[c, :, :, cols].reshape(rank, 2 * VDIM)
                v = jnp.dot(lat, w, preferred_element_type=jnp.float32)
                vbuf[at, cols] = v.astype(jnp.bfloat16)
            return carry

        lax.fori_loop(0, 2, rows_of, 0)

    scale = LOG2E / math.sqrt(QK)

    def attend(c, first_tile, last_tile):
        def tile(j, carry):
            at = pl.ds(pl.multiple_of(j * tok, tok), span)
            hide = bias[j]
            for h in range(chunk_heads):
                begin = (h // 2) * 2 * QK + (h % 2) * NOPE
                q = qbuf[c, j, :, begin:begin + 2 * NOPE]
                s = lax.dot_general(
                    q, kaug[h, at, :], (((1,), (1,)), ((), ())),
                    preferred_element_type=jnp.float32,
                )
                s = s * scale + hide
                peak = jnp.max(s, axis=1, keepdims=True)
                expo = jnp.exp2(s - peak)
                total = jnp.sum(expo, axis=1, keepdims=True)
                cols = slice(h * VDIM, (h + 1) * VDIM)
                mixed = jnp.dot(
                    expo.astype(jnp.bfloat16), vbuf[at, cols],
                    preferred_element_type=jnp.float32,
                )
                obuf[c, j, :, cols] = (mixed / total).astype(jnp.bfloat16)
            return carry

        lax.fori_loop(first_tile, last_tile, tile, 0)

    def q_in(c):
        for k in range(n_head):
            sender = (head + k) % n_head
            landed = qbuf.at[c, sender]
            pltpu.make_async_copy(landed, landed, q_sem.at[c, sender]).wait()

    def give(c):
        for k in range(1, n_head):
            o_copy(c, k).start()
        o_own(c).start()

    def work_on(c):
        middle = n_head // 2

        def tiles_first():
            q_in(c)
            attend(c, 0, middle)

        def tiles_last():
            attend(c, middle, n_head)
            give(c)

        return [functools.partial(project, c), tiles_first, tiles_last]

    waiting = []
    for base in range(0, chunks, 2):
        pair = range(base, min(base + 2, chunks))
        for t in range(1, half + 1):
            for c in pair:
                ring_take(c, t)
                if t == half - 1 and c == pair[-1]:
                    for ahead in range(base + 2, min(base + 4, chunks)):
                        ring_start(ahead, 1)
                if base == 0 and t == 1 and c == pair[-1]:
                    lat_all_in()
                    rope_in()
                if waiting:
                    waiting.pop(0)()
        for c in pair:
            waiting += work_on(c)
    for step in waiting:
        step()

    for c in range(chunks):
        for k in range(n_head):
            sender = (head + k) % n_head
            landed = out.at[:, pl.ds(pl.multiple_of(sender * chunks * cw + c * cw, 128), cw)]
            pltpu.make_async_copy(landed, landed, o_sem.at[c, sender]).wait()
        for k in range(1, n_head):
            q_copy(c, k).wait_send()
            o_copy(c, k).wait_send()
        for t in range(1, half + 1):
            for way, kv in ring_parts(t):
                ring_copy(c, t, way, kv).wait_send()
    for k in range(1, xs):
        lat_copy(k, seq, look + head).wait_send()

    @pl.when(head >= n_head - look)
    def _():
        for k in range(xs):
            lat_copy(xs + k, next_seq, head - (n_head - look)).wait_send()

    for i in range(slots // 2):
        mate_copy(i).wait_send()


def shards(queries, latent, rope_keys, key_weight, value_weight, doc_lengths):
    n_seq, n_head = lax.axis_size("seq"), lax.axis_size("head")
    tok, rank = latent.shape
    rows = key_weight.shape[0]
    local_heads = key_weight.shape[1] // NOPE
    docs = doc_lengths.shape[0]
    slot_rows = n_seq * n_head * tok // docs
    look = 2 * -(-slot_rows // tok)
    chunk_heads = min(4, local_heads)
    chunks = local_heads // chunk_heads
    slots, span, half = look + n_head, (look + 1) * tok, n_seq // 2
    cw, qw = chunk_heads * NOPE, chunk_heads * QK
    latrope = jnp.concatenate(
        [latent, rope_keys, jnp.zeros((tok, 2 * ROPE - rope_keys.shape[1]), latent.dtype)], axis=1
    )
    anywhere = pl.BlockSpec(memory_space=pl.ANY)
    dma = pltpu.SemaphoreType.DMA
    bf16 = jnp.bfloat16
    return pl.pallas_call(
        functools.partial(kernel, (n_seq, n_head, look, chunks, chunk_heads)),
        out_shape=jax.ShapeDtypeStruct((tok, n_head * local_heads * VDIM), bf16),
        in_specs=[anywhere] * 4 + [pl.BlockSpec(memory_space=pltpu.VMEM)],
        out_specs=anywhere,
        scratch_shapes=[
            pltpu.VMEM((slots, tok, rank + 2 * ROPE), bf16),
            pltpu.VMEM((chunks, n_seq, rows, cw), bf16),
            pltpu.VMEM((chunks, n_seq, rows, cw), bf16),
            pltpu.VMEM((chunks, n_head, tok, qw), bf16),
            pltpu.VMEM((chunk_heads, slots * tok, 2 * NOPE), bf16),
            pltpu.VMEM((slots * tok, cw), bf16),
            pltpu.VMEM((n_head, tok, span), jnp.float32),
            pltpu.VMEM((chunks, n_head, tok, cw), bf16),
            dma((slots,)),
            dma((n_head,)),
            dma((slots // 2,)),
            dma((chunks, n_head)),
            dma((chunks, n_head - 1)),
            dma((chunks, 2)),
            dma((chunks, half, 2, 2)),
            dma((chunks, half, 2, 2)),
            dma((chunks, n_head)),
            dma((chunks, n_head - 1)),
        ],
        compiler_params=pltpu.CompilerParams(collective_id=0, has_side_effects=True),
    )(queries, latrope, key_weight, value_weight, doc_lengths.reshape(docs, 1))


def solution(mesh):
    placed = (
        P(("seq", "head"), None),
        P(("seq", "head"), None),
        P(("seq", "head"), None),
        P("seq", "head"),
        P("seq", "head"),
        P(),
    )
    return jax.shard_map(
        shards, mesh=mesh, in_specs=placed, out_specs=P(("seq", "head"), None), check_vma=False
    )
```

```python
import functools
import math

import jax
import jax.numpy as jnp
from jax import lax
from jax.experimental import pallas as pl
from jax.experimental.pallas import tpu as pltpu
from jax.sharding import PartitionSpec as P

NOPE = 128
ROPE = 64
VDIM = 128
QK = NOPE + ROPE
LOG2E = 1.4426950408889634

MESH = pl.DeviceIdType.MESH


def kernel(
    sizes, queries, latent, rope_keys, key_weight, value_weight, lengths, out,
    lat_all, rope_all, wk, wv, qbuf, kaug, vbuf, bias, obuf,
    lat_sem, lat_send, mate_send, x_send, q_sem, q_send, w_own, w_recv, w_send, o_sem, o_send,
):
    n_seq, n_head, look, wide, chunk_heads = sizes
    tok, rank = latent.shape
    rows = key_weight.shape[0]
    half = n_seq // 2
    xs = n_head // 2
    slots = look + n_head
    span = (look + 1) * tok
    cw = chunk_heads * NOPE
    qw = chunk_heads * QK
    pieces = wide + xs
    q_all, o_all = (wide + 1) * qw, (wide + 1) * cw
    seq, head = lax.axis_index("seq"), lax.axis_index("head")
    core, x = head % 2, head // 2
    mate = head + 1 - 2 * core

    odd = seq % 2
    place = (seq // 2) * (1 - odd) + (n_seq - 1 - seq // 2) * odd

    def at_place(where):
        where = (where + n_seq) % n_seq
        fold = where // half
        return 2 * where * (1 - fold) + (2 * (n_seq - 1 - where) + 1) * fold

    after, before = at_place(place + 1), at_place(place - 1)
    next_seq, last_seq = (seq + 1) % n_seq, (seq + n_seq - 1) % n_seq

    barrier = pltpu.get_barrier_semaphore()

    def greet(to_seq, to_head):
        pl.semaphore_signal(barrier, inc=1, device_id=(to_seq, to_head), device_id_type=MESH)

    for k in range(1, n_head):
        greet(seq, (head + k) % n_head)
    greet(after, head)
    greet(before, head)
    for k in range(xs):
        greet(next_seq, ((x + k) % xs) * 2 + core)
        greet(last_seq, ((x + k) % xs) * 2 + core)

    def owner(k, side):
        return ((x + k) % xs) * 2 + side

    def q_cols(who, c):
        return pl.ds(pl.multiple_of(who * q_all + c * qw, 128), qw)

    def o_cols(who, c):
        return pl.ds(pl.multiple_of(who * o_all + c * cw, 128), cw)

    def own_copies():
        mine = look + head
        pltpu.make_async_copy(latent, lat_all.at[mine], lat_sem.at[mine, 0]).start()
        pltpu.make_async_copy(rope_keys, rope_all.at[mine], lat_sem.at[mine, 1]).start()
        for c in range(wide + 1):
            for kv, (source, held) in enumerate(((key_weight, wk), (value_weight, wv))):
                pltpu.make_async_copy(
                    source.at[:, pl.ds(c * cw, cw)], held.at[c, seq], w_own.at[c, kv]
                ).start()
        for c in range(wide):
            pltpu.make_async_copy(
                queries.at[:, q_cols(head, c)], qbuf.at[c, head], q_sem.at[c, head]
            ).start()
        for k in range(xs):
            pltpu.make_async_copy(
                queries.at[:, q_cols(owner(k, core), wide)],
                qbuf.at[wide + k, core], q_sem.at[wide + k, core],
            ).start()

    own_copies()
    pl.semaphore_wait(barrier, n_head - 1 + 2 + 2 * xs)

    def lat_copies(k, to_seq, slot):
        return [
            pltpu.make_async_remote_copy(
                src_ref=source, dst_ref=held.at[slot],
                send_sem=lat_send.at[k, part], recv_sem=lat_sem.at[slot, part],
                device_id=(to_seq, ((x + k % xs) % xs) * 2 + core), device_id_type=MESH,
            )
            for part, (source, held) in enumerate(((latent, lat_all), (rope_keys, rope_all)))
        ]

    def x_copies(k):
        return [
            pltpu.make_async_remote_copy(
                src_ref=source.at[:, pl.ds(wide * cw, cw)], dst_ref=held.at[wide + k, seq],
                send_sem=x_send.at[k - 1, kv], recv_sem=w_own.at[wide + k, kv],
                device_id=(seq, ((x + xs - k) % xs) * 2 + core), device_id_type=MESH,
            )
            for kv, (source, held) in enumerate(((key_weight, wk), (value_weight, wv)))
        ]

    def ring_parts(t):
        both = [(0, 0), (0, 1), (1, 0), (1, 1)]
        return both if t < half else [(0, 0), (1, 1)]

    def own_weights(c):
        for kv in range(2):
            mine = (wk, wv)[kv].at[c, seq]
            pltpu.make_async_copy(mine, mine, w_own.at[c, kv]).wait()

    def ring_copy(c, t, way, kv):
        origin = at_place(place - (t - 1)) if way == 0 else at_place(place + (t - 1))
        source, held = ((key_weight, wk), (value_weight, wv))[kv]
        src = source.at[:, pl.ds(c * cw, cw)] if t == 1 and c <= wide else held.at[c, origin]
        index = t - 1
        return pltpu.make_async_remote_copy(
            src_ref=src, dst_ref=held.at[c, origin],
            send_sem=w_send.at[c, index, way, kv], recv_sem=w_recv.at[c, index, way, kv],
            device_id=(after if way == 0 else before, head), device_id_type=MESH,
        )

    def ring_start(c, t):
        if c > wide:
            own_weights(c)
        for way, kv in ring_parts(t):
            ring_copy(c, t, way, kv).start()

    def ring_take(c, t):
        for way, kv in ring_parts(t):
            origin = at_place(place - t) if way == 0 else at_place(place + t)
            landed = (wk, wv)[kv].at[c, origin]
            pltpu.make_async_copy(landed, landed, w_recv.at[c, t - 1, way, kv]).wait()
            if t + 1 <= half and (way, kv) in ring_parts(t + 1):
                ring_copy(c, t + 1, way, kv).start()

    def q_copies(c):
        if c < wide:
            routes = [((head + k) % n_head,) * 2 + (head,) for k in range(1, n_head)]
        else:
            routes = [(mate, owner(c - wide, 1 - core), core)]
        return [
            pltpu.make_async_remote_copy(
                src_ref=queries.at[:, q_cols(who, min(c, wide))], dst_ref=qbuf.at[c, slot],
                send_sem=q_send.at[c, k], recv_sem=q_sem.at[c, slot],
                device_id=(seq, peer), device_id_type=MESH,
            )
            for k, (peer, who, slot) in enumerate(routes)
        ]

    def o_copies(c):
        if c < wide:
            routes = [((head + k) % n_head,) * 2 + (head, head) for k in range(1, n_head)]
        else:
            routes = [(mate, 1 - core, owner(c - wide, core), core)]
        return [
            pltpu.make_async_remote_copy(
                src_ref=obuf.at[c, tile], dst_ref=out.at[:, o_cols(who, min(c, wide))],
                send_sem=o_send.at[c, k], recv_sem=o_sem.at[c, slot],
                device_id=(seq, peer), device_id_type=MESH,
            )
            for k, (peer, tile, who, slot) in enumerate(routes)
        ]

    def o_own(c):
        if c < wide:
            tile, who, slot = head, head, head
        else:
            tile, who, slot = core, owner(c - wide, core), core
        return pltpu.make_async_copy(
            obuf.at[c, tile], out.at[:, o_cols(who, min(c, wide))], o_sem.at[c, slot]
        )

    for k in range(1, xs):
        for copy in lat_copies(k, seq, look + head):
            copy.start()

    @pl.when(head >= n_head - look)
    def _():
        for k in range(xs):
            for copy in lat_copies(xs + k, next_seq, head - (n_head - look)):
                copy.start()

    groups = [list(range(wide)), list(range(wide, pieces))]
    for c in groups[0]:
        ring_start(c, 1)
    for c in range(pieces):
        for copy in q_copies(c):
            copy.start()
        if c == 0:
            for k in range(1, xs):
                for copy in x_copies(k):
                    copy.start()

    docs = lengths.shape[0]
    first = seq * n_head * tok

    def mask_tile(j, carry):
        q_place = first + j * tok + lax.broadcasted_iota(jnp.int32, (tok, 1), 0)

        def document(d, state):
            start, begun = state
            return start + lengths[d], jnp.where(start <= q_place, start, begun)

        _, begun = lax.fori_loop(
            0, docs, document, (jnp.int32(0), jnp.zeros((tok, 1), jnp.int32)), unroll=True
        )
        k_place = first + (j - look) * tok + lax.broadcasted_iota(jnp.int32, (tok, span), 1)
        seen = (k_place >= begun) & (k_place <= q_place)
        bias[j] = jnp.where(seen, 0.0, -jnp.inf)
        return carry

    lax.fori_loop(0, n_head, mask_tile, 0)

    def lat_wait(slot):
        for part, held in enumerate((lat_all, rope_all)):
            pltpu.make_async_copy(held.at[slot], held.at[slot], lat_sem.at[slot, part]).wait()

    def mate_copies(i):
        slot = 2 * i + core
        return [
            pltpu.make_async_remote_copy(
                src_ref=held.at[slot], dst_ref=held.at[slot],
                send_sem=mate_send.at[i, part], recv_sem=lat_sem.at[slot, part],
                device_id=(seq, mate), device_id_type=MESH,
            )
            for part, held in enumerate((lat_all, rope_all))
        ]

    def lat_all_in():
        for i in list(range(look // 2, slots // 2)) + list(range(look // 2)):
            lat_wait(2 * i + core)
            for copy in mate_copies(i):
                copy.start()
        for i in range(slots // 2):
            lat_wait(2 * i + 1 - core)

    def rope_in():
        first_half = lax.broadcasted_iota(jnp.int32, (tok, 2 * ROPE), 1) < ROPE

        def fill(slot, carry):
            rope = rope_all[slot].astype(jnp.float32)
            twice = jnp.concatenate([rope, rope], axis=1)
            at = pl.ds(pl.multiple_of(slot * tok, tok), tok)
            for h in range(chunk_heads):
                shown = jnp.where(first_half, twice, 0.0) if h % 2 == 0 else twice
                kaug[h, at, NOPE:] = shown.astype(jnp.bfloat16)
            return carry

        lax.fori_loop(0, slots, fill, 0)

    block = 2 * tok

    def project(c):
        if c <= wide:
            own_weights(c)
        first_slot, blocks = (0, slots // 2) if c < wide else (2 * x, (look + 2) // 2)

        def rows_of(i, carry):
            slot = first_slot + 2 * i
            at = pl.ds(pl.multiple_of(slot * tok, tok), block)
            lat = lat_all[pl.ds(slot, 2)].reshape(block, rank)
            low = lax.broadcasted_iota(jnp.int32, (block, NOPE), 1) < ROPE
            for pair in range(chunk_heads // 2):
                cols = slice(pair * 2 * NOPE, (pair + 1) * 2 * NOPE)
                w = wk[c, :, :, cols].reshape(rank, 2 * NOPE)
                k = jnp.dot(lat, w, preferred_element_type=jnp.float32)
                kaug[2 * pair, at, :NOPE] = k[:, :NOPE].astype(jnp.bfloat16)
                turned = pltpu.roll(k[:, NOPE:], ROPE, axis=1)
                zeros_first = jnp.where(low, 0.0, turned).astype(jnp.bfloat16)
                kaug[2 * pair + 1, at, :NOPE] = zeros_first
                rope_last = kaug[2 * pair + 1, at, NOPE:].astype(jnp.float32)
                kaug[2 * pair + 1, at, NOPE:] = jnp.where(low, turned, rope_last).astype(
                    jnp.bfloat16
                )
                w = wv[c, :, :, cols].reshape(rank, 2 * VDIM)
                v = jnp.dot(lat, w, preferred_element_type=jnp.float32)
                vbuf[at, cols] = v.astype(jnp.bfloat16)
            return carry

        lax.fori_loop(0, blocks, rows_of, 0)

    scale = LOG2E / math.sqrt(QK)

    def attend(c, first_tile, last_tile):
        def tile(j, carry):
            place_of = j if c < wide else 2 * x + j
            at = pl.ds(pl.multiple_of(place_of * tok, tok), span)
            hide = bias[place_of]
            for h in range(chunk_heads):
                begin = (h // 2) * 2 * QK + (h % 2) * NOPE
                q = qbuf[c, j, :, begin:begin + 2 * NOPE]
                s = lax.dot_general(
                    q, kaug[h, at, :], (((1,), (1,)), ((), ())),
                    preferred_element_type=jnp.float32,
                )
                s = s * scale + hide
                peak = jnp.max(s, axis=1, keepdims=True)
                expo = jnp.exp2(s - peak)
                total = jnp.sum(expo, axis=1, keepdims=True)
                cols = slice(h * VDIM, (h + 1) * VDIM)
                mixed = jnp.dot(
                    expo.astype(jnp.bfloat16), vbuf[at, cols],
                    preferred_element_type=jnp.float32,
                )
                obuf[c, j, :, cols] = (mixed / total).astype(jnp.bfloat16)
            return carry

        lax.fori_loop(first_tile, last_tile, tile, 0)

    def q_in(c):
        for slot in range(n_head if c < wide else 2):
            landed = qbuf.at[c, slot]
            pltpu.make_async_copy(landed, landed, q_sem.at[c, slot]).wait()

    def give(c):
        for copy in o_copies(c):
            copy.start()
        o_own(c).start()

    def work_on(c):
        tiles = n_head if c < wide else 2

        def tiles_first():
            q_in(c)
            attend(c, 0, tiles // 2)

        def tiles_last():
            attend(c, tiles // 2, tiles)
            give(c)

        return [functools.partial(project, c), tiles_first, tiles_last]

    waiting = []
    for number, group in enumerate(groups):
        for t in range(1, half + 1):
            for c in group:
                ring_take(c, t)
                if t == half - 1 and c == group[-1] and number + 1 < len(groups):
                    for ahead in groups[number + 1]:
                        ring_start(ahead, 1)
                if number == 0 and t == 1 and c == group[-1]:
                    lat_all_in()
                    rope_in()
                if t == half:
                    waiting += work_on(c)
                for _ in range(min(1, len(waiting))):
                    waiting.pop(0)()
    for step in waiting:
        step()

    for c in range(pieces):
        for slot in range(n_head if c < wide else 2):
            who = slot if c < wide else owner(c - wide, slot)
            landed = out.at[:, o_cols(who, min(c, wide))]
            pltpu.make_async_copy(landed, landed, o_sem.at[c, slot]).wait()
        for copy in q_copies(c) + o_copies(c):
            copy.wait_send()
        for t in range(1, half + 1):
            for way, kv in ring_parts(t):
                ring_copy(c, t, way, kv).wait_send()
    for k in range(1, xs):
        for copy in lat_copies(k, seq, look + head) + x_copies(k):
            copy.wait_send()

    @pl.when(head >= n_head - look)
    def _():
        for k in range(xs):
            for copy in lat_copies(xs + k, next_seq, head - (n_head - look)):
                copy.wait_send()

    for i in range(slots // 2):
        for copy in mate_copies(i):
            copy.wait_send()


def shards(queries, latent, rope_keys, key_weight, value_weight, doc_lengths):
    n_seq, n_head = lax.axis_size("seq"), lax.axis_size("head")
    tok, rank = latent.shape
    rows = key_weight.shape[0]
    local_heads = key_weight.shape[1] // NOPE
    docs = doc_lengths.shape[0]
    slot_rows = n_seq * n_head * tok // docs
    look = 2 * -(-slot_rows // tok)
    chunk_heads = min(4, local_heads)
    wide = local_heads // chunk_heads - 1
    pieces = wide + n_head // 2
    slots, span, half = look + n_head, (look + 1) * tok, n_seq // 2
    cw, qw = chunk_heads * NOPE, chunk_heads * QK
    anywhere = pl.BlockSpec(memory_space=pl.ANY)
    dma = pltpu.SemaphoreType.DMA
    bf16 = jnp.bfloat16
    return pl.pallas_call(
        functools.partial(kernel, (n_seq, n_head, look, wide, chunk_heads)),
        out_shape=jax.ShapeDtypeStruct((tok, n_head * local_heads * VDIM), bf16),
        in_specs=[anywhere] * 5 + [pl.BlockSpec(memory_space=pltpu.SMEM)],
        out_specs=anywhere,
        scratch_shapes=[
            pltpu.VMEM((slots, tok, rank), bf16),
            pltpu.VMEM((slots, tok, ROPE), bf16),
            pltpu.VMEM((pieces, n_seq, rows, cw), bf16),
            pltpu.VMEM((pieces, n_seq, rows, cw), bf16),
            pltpu.VMEM((pieces, n_head, tok, qw), bf16),
            pltpu.VMEM((chunk_heads, slots * tok, 2 * NOPE), bf16),
            pltpu.VMEM((slots * tok, cw), bf16),
            pltpu.VMEM((n_head, tok, span), jnp.float32),
            pltpu.VMEM((pieces, n_head, tok, cw), bf16),
            dma((slots, 2)),
            dma((n_head, 2)),
            dma((slots // 2, 2)),
            dma((n_head // 2 - 1, 2)),
            dma((pieces, n_head)),
            dma((pieces, n_head - 1)),
            dma((pieces, 2)),
            dma((pieces, half, 2, 2)),
            dma((pieces, half, 2, 2)),
            dma((pieces, n_head)),
            dma((pieces, n_head - 1)),
        ],
        compiler_params=pltpu.CompilerParams(collective_id=0, has_side_effects=True),
    )(queries, latent, rope_keys, key_weight, value_weight, doc_lengths)


def solution(mesh):
    placed = (
        P(("seq", "head"), None),
        P(("seq", "head"), None),
        P(("seq", "head"), None),
        P("seq", "head"),
        P("seq", "head"),
        P(),
    )
    return jax.shard_map(
        shards, mesh=mesh, in_specs=placed, out_specs=P(("seq", "head"), None), check_vma=False
    )
```
